512 devices in a mesh: member: 2 (over y), tile: 32 (over z), row: 4 (over x), lev: 2 (over core).
Axes of the slice: x: 4, y: 2, z: 32, core: 2. Of those that a mesh axis runs over, the one named last changes fastest.
The devices are a block of a 4x8x32 slice.
Arguments:
- thickness: float32 [128, 512, 512], P(('member', 'lev'), 'tile', 'row'), parts along dimension 0, may hold values from 0.24 to 14.91
- zonal_wind: float32 [128, 512, 512], P(('member', 'lev'), 'tile', 'row'), parts along dimension 0, may hold values from -1.8 to 1.8
- merid_wind: float32 [128, 512, 512], P(('member', 'lev'), 'tile', 'row'), parts along dimension 0, may hold values from -1.8 to 1.8
- pert_codes: int32 [1024, 512], P(('member', 'tile'), 'row'), parts along dimension 0, may hold values from 0 to 1073741823
Outputs:
- thick_out: float32 [128, 512, 512], P(('member', 'lev'), 'tile', 'row'), parts along dimension 0
- zonal_out: float32 [128, 512, 512], P(('member', 'lev'), 'tile', 'row'), parts along dimension 0
- merid_out: float32 [128, 512, 512], P(('member', 'lev'), 'tile', 'row'), parts along dimension 0
The draws below stay inside these ranges and needn't reach their ends.
There are 2 independent parts, one for each index of `member`. The reference program is written for one: setup_inputs(seed, part) draws one part's arguments, and reference() takes and returns one part's arrays. A program takes and returns all parts, laid end to end along the dimension named above; each array names one. Nothing has to cross between parts.
All inputs are finite; a program needn't handle non-finite values.
Results may differ from the reference program's by a relative error of at most 0.0003.
Values sent between devices are 32-bit elements; how exact they have to be, the bound alone decides.
A program may use at most 64 MiB of HBM per device.

```python
import math
import jax
import jax.numpy as jnp
from jax import lax

NZ = 64
NSUB = 4
NX = 512
NY = 512


def draw_thickness(key, part):
    scale_key = jax.random.fold_in(key, 11)
    rough_key = jax.random.fold_in(key, 23)
    region_draw = jax.random.uniform(scale_key, (8, 2), jnp.float32, 0.0, 1.0)
    region_scale = jnp.exp(math.log(0.35) + math.log(10.0) * region_draw)
    region_first = (jnp.arange(NX) * 8 // NX).astype(jnp.int32)
    region_second = (jnp.arange(NY) * 2 // NY).astype(jnp.int32)
    cell_scale = jnp.take(jnp.take(region_scale, region_first, axis=0), region_second, axis=1)
    across = jnp.arange(NX).astype(jnp.float32) / max(NX - 1, 1)
    base = (1.0 + 2.0 * across[:, None]) * cell_scale
    rough = jax.random.uniform(rough_key, (NZ, NX, NY), jnp.float32, -0.35, 0.35)
    return (base[None] * jnp.exp(rough)).astype(jnp.float32)


def place_ends(array, stream_key, smallest, high):
    longest = array.shape.index(max(array.shape))
    spots = []
    for shift in (0, 1):
        where = [jax.random.randint(jax.random.fold_in(stream_key, axis), (), 0, length) for axis, length in enumerate(array.shape)]
        where[longest] = (where[longest] + shift) % array.shape[longest]
        spots.append(tuple(where))
    return array.at[spots[0]].set(smallest).at[spots[1]].set(high)


def shard_levels(key, extent, cuts, least, high):
    level = 1.0
    for position, blocks in cuts:
        draws = jax.random.uniform(jax.random.fold_in(jax.random.fold_in(key, 6), position), (blocks,), jnp.float32, least / len(cuts), high / len(cuts))
        level = level * jnp.repeat(jnp.exp(draws), extent[position] // blocks).reshape((-1,) + (1,) * (len(extent) - 1 - position))
    return level


def centred(rng, extent, deviation, bound, shards=(), held_as=jnp.bfloat16):
    loudness = shard_levels(rng, extent, shards, -0.22, 0.18) if shards else 1.0
    drawn = jax.random.normal(rng, extent, jnp.float32) * deviation * loudness
    return jnp.minimum(jnp.maximum(drawn, -bound), bound).astype(held_as)


def setup_inputs(seed: int = 0, part: int = 0) -> dict:
    splits = jax.random.split(jax.random.key(seed), 5)
    part_splits = jax.random.split(jax.random.fold_in(splits[4], part), 5)
    thickness = draw_thickness(jax.random.fold_in(jax.random.fold_in(splits[4], part), 71), part)
    zonal_wind = centred(part_splits[1], (NZ, NX, NY), 0.3, 1.8, ((0, 2), (1, 32), (2, 4)), jnp.float32)
    merid_wind = centred(part_splits[2], (NZ, NX, NY), 0.3, 1.8, ((0, 2), (1, 32), (2, 4)), jnp.float32)
    pert_codes = place_ends(jax.random.randint(part_splits[3], (NX, NY), 0, 1073741824), jax.random.fold_in(part_splits[3], 1), 0, 1073741823).astype(jnp.int32)
    return dict(thickness=thickness, zonal_wind=zonal_wind, merid_wind=merid_wind, pert_codes=pert_codes)


CFL_NUMBER = 0.8

def advance(stacked, half_step):
    height = stacked[0]
    zonal = stacked[1]
    merid = stacked[2]
    zonal_new = zonal[:, 1:-1, 1:-1] - half_step * (height[:, 2:, 1:-1] - height[:, :-2, 1:-1])
    merid_new = merid[:, 1:-1, 1:-1] - half_step * (height[:, 1:-1, 2:] - height[:, 1:-1, :-2])
    centre = height[:, 1:-1, 1:-1]
    flux_east = centre * zonal_new
    flux_north = centre * merid_new
    height_new = centre[:, 1:-1, 1:-1] - half_step * (flux_east[:, 2:, 1:-1] - flux_east[:, :-2, 1:-1] + (flux_north[:, 1:-1, 2:] - flux_north[:, 1:-1, :-2]))
    return jnp.stack([height_new, zonal_new[:, 1:-1, 1:-1], merid_new[:, 1:-1, 1:-1]])

def reference(thickness, zonal_wind, merid_wind, pert_codes):
    bump = 2.0 * (pert_codes % 4096).astype(jnp.float32) / 4095.0
    raised = thickness + bump[None]
    peak = jnp.max(raised)
    base_mass = jnp.sum(thickness)
    raised_mass = jnp.sum(raised)
    height = raised * (base_mass / raised_mass)
    half_step = 0.5 * CFL_NUMBER / jnp.sqrt(peak)
    state = jnp.stack([height, zonal_wind, merid_wind])
    for substep in range(NSUB):
        padded = jnp.pad(state, ((0, 0), (0, 0), (2, 2), (2, 2)), mode='wrap')
        state = advance(padded, half_step)
    height = state[0]
    zonal = state[1]
    merid = state[2]
    total = lax.optimization_barrier(jnp.sum(height, 0))
    tops = jnp.cumsum(height, 0) - height
    levels = height.shape[0]

    def integral(mark):
        target = total * (mark / levels)
        over = jnp.clip(target[None] - tops, 0.0, height)
        return (lax.optimization_barrier(jnp.sum(zonal * over, 0)), lax.optimization_barrier(jnp.sum(merid * over, 0)))
    marks = jnp.arange(levels + 1).astype(jnp.int32).astype(jnp.float32)
    zonal_sum, merid_sum = lax.map(integral, marks)
    layer = total / levels
    thick_out = jnp.broadcast_to(layer, (levels,) + layer.shape)
    zonal_out = (zonal_sum[1:] - zonal_sum[:-1]) / layer
    merid_out = (merid_sum[1:] - merid_sum[:-1]) / layer
    return (thick_out, zonal_out, merid_out)
```

```python
import functools
import jax
import jax.numpy as jnp
from jax import lax
from jax.experimental import pallas as pl
from jax.experimental.pallas import tpu as pltpu
from jax.sharding import PartitionSpec as P

NSUB = 4


CFL_NUMBER = 0.8

MESH = pl.DeviceIdType.MESH


def combine(lane, a, b):
    return jnp.where(lane == 0, jnp.maximum(a, b), a + b)


def totals_kernel(
    tiles, rows, thick_ref, codes_ref, out_ref,
    mine, plane, near, far, got_plane, got_near, got_mid, got_far,
    send_plane, recv_plane, send_near, recv_near, send_mid, recv_mid, send_far, recv_far,
):
    tile = lax.axis_index("tile")
    row = lax.axis_index("row")
    lev = lax.axis_index("lev")

    def along(d):
        return lax.rem(tile + (d + tiles), tiles)

    def mate(dr, dl):
        return {"row": lax.rem(row + dr, rows), "lev": lax.rem(lev + dl, 2)}

    mates = [(dr, dl) for dr in range(rows) for dl in range(2) if dr or dl]
    close = [1, -1, 2, -2, 3, -3]

    barrier = pltpu.get_barrier_semaphore()
    for dr, dl in mates:
        pl.semaphore_signal(barrier, inc=1, device_id=mate(dr, dl), device_id_type=MESH)
    for d in close:
        pl.semaphore_signal(barrier, inc=1, device_id={"tile": along(d)}, device_id_type=MESH)

    thick = thick_ref[...]
    bump = 2.0 * (codes_ref[...] & 4095).astype(jnp.float32) / 4095.0
    raised = thick + bump[None]

    def folded(x, op):
        x = op(x, axis=0)
        x = op(x, axis=0, keepdims=True)
        return op(x, axis=1, keepdims=True)

    lane = lax.broadcasted_iota(jnp.int32, (1, 128), 1)
    peak = folded(raised, jnp.max)
    base = folded(thick, jnp.sum)
    lifted = folded(raised, jnp.sum)
    packet = jnp.where(lane == 0, peak, jnp.where(lane == 1, base, lifted))
    mine[0] = packet
    pl.semaphore_wait(barrier, len(mates) + len(close))

    copies = []

    def send(src, dst, ssem, rsem, device):
        copy = pltpu.make_async_remote_copy(
            src_ref=src, dst_ref=dst, send_sem=ssem, recv_sem=rsem,
            device_id=device, device_id_type=MESH,
        )
        copy.start()
        copies.append(copy)

    for s, (dr, dl) in enumerate(mates):
        send(mine.at[0], got_plane.at[s], send_plane.at[s], recv_plane.at[s], mate(dr, dl))
    total = packet
    for s in range(len(mates)):
        copies[s].wait_recv()
        total = combine(lane, total, got_plane[s])
    plane[0] = total

    first = len(copies)
    for s, d in enumerate(close):
        send(plane.at[0], got_near.at[s], send_near.at[s], recv_near.at[s], {"tile": along(d)})
    held = {0: total}
    for s, d in enumerate(close):
        copies[first + s].wait_recv()
        held[-d] = got_near[s]

    def over(lo, hi):
        out = held[lo]
        for i in range(lo + 1, hi + 1):
            out = combine(lane, out, held[i])
        return out

    up = over(-3, 2)
    down = over(-2, 2)
    near[0] = up
    near[1] = jnp.where(lane < 3, down, pltpu.roll(held[3], 3, 1))
    first = len(copies)
    send(near.at[0], got_mid.at[0], send_mid.at[0], recv_mid.at[0], {"tile": along(6)})
    send(near.at[1], got_mid.at[1], send_mid.at[1], recv_mid.at[1], {"tile": along(-6)})
    copies[first].wait_recv()
    copies[first + 1].wait_recv()
    below = got_mid[0]
    above = got_mid[1]
    above_last = pltpu.roll(above, 125, 1)

    far[0] = combine(lane, below, held[-3])
    far[1] = combine(lane, above, held[3])
    first = len(copies)
    send(far.at[0], got_far.at[0], send_far.at[0], recv_far.at[0], {"tile": along(7)})
    send(far.at[1], got_far.at[1], send_far.at[1], recv_far.at[1], {"tile": along(-7)})
    inner = combine(lane, over(-3, 3), combine(lane, below, combine(lane, above, above_last)))
    copies[first].wait_recv()
    copies[first + 1].wait_recv()
    out_ref[...] = combine(lane, inner, combine(lane, got_far[0], got_far[1]))
    for copy in copies:
        copy.wait_send()


def totals(thickness, pert_codes):
    tiles = lax.axis_size("tile")
    rows = lax.axis_size("row")
    mates = 2 * rows - 1
    dma = pltpu.SemaphoreType.DMA
    packets = lambda n: pltpu.VMEM((n, 1, 128), jnp.float32)
    return pl.pallas_call(
        functools.partial(totals_kernel, tiles, rows),
        out_shape=jax.ShapeDtypeStruct((1, 128), jnp.float32),
        in_specs=[pl.BlockSpec(memory_space=pltpu.VMEM)] * 2,
        out_specs=pl.BlockSpec(memory_space=pltpu.VMEM),
        scratch_shapes=[
            packets(1), packets(1), packets(2), packets(2),
            packets(mates), packets(6), packets(2), packets(2),
            dma((mates,)), dma((mates,)), dma((6,)), dma((6,)), dma((2,)), dma((2,)), dma((2,)), dma((2,)),
        ],
        compiler_params=pltpu.CompilerParams(collective_id=0, has_side_effects=True),
        name="totals",
    )(thickness, pert_codes)


def padded(block, sides, width):
    for axis, dim in sides:
        count = lax.axis_size(axis)
        forward = [(i, i + 1) for i in range(count - 1)]
        forward.append((count - 1, 0))
        backward = [(target, source) for source, target in forward]
        low = lax.ppermute(
            lax.slice_in_dim(block, block.shape[dim] - width, None, axis=dim), axis, forward
        )
        high = lax.ppermute(lax.slice_in_dim(block, 0, width, axis=dim), axis, backward)
        block = jnp.concatenate([low, block, high], axis=dim)
    return block


def joined_along(pieces, dim):
    pieces = jnp.moveaxis(pieces, 0, dim)
    dims = pieces.shape
    return pieces.reshape(*dims[:dim], dims[dim] * dims[dim + 1], *dims[dim + 2 :])


def sent_to_all(shard, axis):
    length = lax.axis_size(axis)
    return lax.all_to_all(
        jnp.broadcast_to(shard[None], (length, *shard.shape)), axis, 0, 0, tiled=True
    )


def gathered_copies(shard, axis, dim):
    return joined_along(sent_to_all(shard, axis), dim)


def advance(stacked, half_step):
    height = stacked[0]
    zonal = stacked[1]
    merid = stacked[2]
    zonal_new = zonal[:, 1:-1, 1:-1] - half_step * (height[:, 2:, 1:-1] - height[:, :-2, 1:-1])
    merid_new = merid[:, 1:-1, 1:-1] - half_step * (height[:, 1:-1, 2:] - height[:, 1:-1, :-2])
    centre = height[:, 1:-1, 1:-1]
    flux_east = centre * zonal_new
    flux_north = centre * merid_new
    height_new = centre[:, 1:-1, 1:-1] - half_step * (
        flux_east[:, 2:, 1:-1]
        - flux_east[:, :-2, 1:-1]
        + (flux_north[:, 1:-1, 2:] - flux_north[:, 1:-1, :-2])
    )
    return jnp.stack([height_new, zonal_new[:, 1:-1, 1:-1], merid_new[:, 1:-1, 1:-1]])


def remap_columns(columns, first, count):
    height = columns[0]
    zonal = columns[1]
    merid = columns[2]
    levels = height.shape[0]
    total = jnp.sum(height, 0)
    tops = jnp.cumsum(height, 0) - height
    marks = (first + jnp.arange(count + 1)).astype(jnp.float32)
    targets = total[None] * (marks / levels)[:, None, None]
    zonal_sum = jnp.zeros(targets.shape, jnp.float32)
    merid_sum = jnp.zeros(targets.shape, jnp.float32)
    for block in range(levels // 8):
        lower = block * 8
        upper = lower + 8
        over = jnp.clip(targets[None] - tops[lower:upper, None], 0.0, height[lower:upper, None])
        zonal_sum = zonal_sum + jnp.sum(zonal[lower:upper, None] * over, 0)
        merid_sum = merid_sum + jnp.sum(merid[lower:upper, None] * over, 0)
    layer = total / levels
    thick_new = jnp.broadcast_to(layer, (count,) + layer.shape)
    zonal_new = (zonal_sum[1:] - zonal_sum[:-1]) / layer
    merid_new = (merid_sum[1:] - merid_sum[:-1]) / layer
    return jnp.stack([thick_new, zonal_new, merid_new])


def local(thickness, zonal_wind, merid_wind, pert_codes):
    bump = 2.0 * (pert_codes % 4096).astype(jnp.float32) / 4095.0
    raised = thickness + bump[None]
    sums = totals(thickness, pert_codes)
    peak, base_total, raised_total = sums[0, 0], sums[0, 1], sums[0, 2]
    height = raised * (base_total / raised_total)
    half_step = 0.5 * CFL_NUMBER / jnp.sqrt(peak)
    state = jnp.stack([height, zonal_wind, merid_wind])
    state = padded(state, (("tile", 2), ("row", 3)), 2 * NSUB)
    for substep in range(NSUB):
        state = advance(state, half_step)
    levels_here = state.shape[1]
    columns = gathered_copies(state, "lev", 1)
    result = remap_columns(columns, lax.axis_index("lev") * levels_here, levels_here)
    return (result[0], result[1], result[2])


def solution(mesh):
    in_specs = (
        P(("member", "lev"), "tile", "row"),
        P(("member", "lev"), "tile", "row"),
        P(("member", "lev"), "tile", "row"),
        P(("member", "tile"), "row"),
    )
    out_specs = (
        P(("member", "lev"), "tile", "row"),
        P(("member", "lev"), "tile", "row"),
        P(("member", "lev"), "tile", "row"),
    )
    return jax.shard_map(local, mesh=mesh, in_specs=in_specs, out_specs=out_specs, check_vma=False)
```
